128 devices in a mesh: sys: 1, col: 2 (over core), seg: 64 (over z, y, x).
Axes of the slice: x: 4, y: 4, z: 4, core: 2. Of those that a mesh axis runs over, the one named last changes fastest.
Arguments:
- positions: bfloat16 [131072, 128], P(('sys', 'seg', 'col'))
- charges: float32 [131072], P(('sys', 'seg', 'col'))
Outputs:
- output 1: float32 [131072, 128], P(('sys', 'seg', 'col'))
- output 2: float32 [1], P('sys')
All inputs are finite; a program needn't handle non-finite values.
Results may differ from the reference program's by a relative error of at most 0.001.
Values are sent between devices in bfloat16 or wider.
A program may use at most 1 GiB of HBM per device.

```python
import jax
import jax.numpy as jnp
from jax import lax

PARTICLES = 131072
FEAT_DIM = 128
ROW_BLOCK = min(PARTICLES, 256)
BLOCK_COUNT = PARTICLES // ROW_BLOCK
INV_LEN2 = 1.0 / FEAT_DIM
CHARGE_SCALE = (2.0 * FEAT_DIM) ** 0.5 * PARTICLES ** -0.25


def setup_inputs(seed: int = 0, part: int = 0) -> dict:
    base_key = jax.random.fold_in(jax.random.key(seed), part)
    key_pos, key_charge = jax.random.split(base_key)
    positions = jax.random.normal(key_pos, (PARTICLES, FEAT_DIM), jnp.float32).astype(jnp.bfloat16)
    charges = CHARGE_SCALE * jax.random.normal(key_charge, (PARTICLES,), jnp.float32)
    return {'positions': positions, 'charges': charges}


def reference(positions, charges):
    pos_wide = positions.astype(jnp.float32)
    sq_norm = jnp.sum(pos_wide * pos_wide, axis=1)
    all_pos = jnp.arange(PARTICLES)

    def one_block(blk_index):
        row_start = blk_index * ROW_BLOCK
        x_rows = lax.dynamic_slice_in_dim(positions, row_start, ROW_BLOCK, 0)
        q_rows = lax.dynamic_slice_in_dim(charges, row_start, ROW_BLOCK, 0)
        s_rows = lax.dynamic_slice_in_dim(sq_norm, row_start, ROW_BLOCK, 0)
        dot_prod = jnp.dot(x_rows, positions.T, preferred_element_type=jnp.float32)
        sq_dist = jnp.maximum(s_rows[:, None] + sq_norm[None, :] - 2.0 * dot_prod, 0.0)
        weights = q_rows[:, None] * charges[None, :] * jnp.exp(-0.5 * INV_LEN2 * sq_dist)
        row_ids = row_start + jnp.arange(ROW_BLOCK)
        weights = jnp.where(row_ids[:, None] == all_pos[None, :], 0.0, weights)
        pulled = jnp.dot(weights.astype(jnp.bfloat16), positions, preferred_element_type=jnp.float32)
        forces = (jnp.sum(weights, axis=1)[:, None] * x_rows.astype(jnp.float32) - pulled) * INV_LEN2
        return forces, jnp.sum(weights)

    forces, energies = lax.map(one_block, jnp.arange(BLOCK_COUNT))
    return forces.reshape(PARTICLES, FEAT_DIM), (0.5 * jnp.sum(energies)).reshape(1)
```

```python
import functools
import math

import jax
import jax.numpy as jnp
from jax import lax
from jax.experimental import pallas as pl
from jax.experimental.pallas import tpu as pltpu
from jax.sharding import PartitionSpec as P

F32 = jnp.float32
BF16 = jnp.bfloat16
ROW_AXES = ('sys', 'seg', 'col')
GA, GT = 16, 8
OWN = 1024
TB = 256
NB = OWN // TB
EXT = 48
PR = 64
NP = TB // PR
HALF_SHELL = GA // 2


def grid_of(seg, col):
    z, y, x = seg // 16, (seg // 4) % 4, seg % 4
    ya = y // 2
    yb = (ya + y % 2) % 2
    return (z * 2 + ya) * 2 + col, x * 2 + yb


def shift_pairs(da, dt):
    at = {grid_of(seg, col): col * 64 + seg for seg in range(64) for col in range(2)}
    return [(at[((a + da) % GA, (t + dt) % GT)], at[(a, t)]) for a in range(GA) for t in range(GT)]


def split3(v):
    hi = lax.reduce_precision(v, 8, 7)
    mid = lax.reduce_precision(v - hi, 8, 7)
    lo = lax.reduce_precision(v - hi - mid, 8, 7)
    return [p.astype(BF16) for p in (hi, mid, lo)]


def pair_kernel(scale, flags, xe, fu, fv, en, xi, xv, xtv, qu, qv, su, sv, *wsc):
    def ext_row(b, m, ib):
        row = xe[b, OWN + 8 * m:OWN + 8 * (m + 1), :].astype(F32)
        sel = lax.broadcasted_iota(jnp.int32, (8, 128), 0)
        lo = jnp.sum(jnp.where(sel == 2 * ib, row, 0.0), axis=0, keepdims=True)
        hi = jnp.sum(jnp.where(sel == 2 * ib + 1, row, 0.0), axis=0, keepdims=True)
        return jnp.concatenate([lo, hi], axis=1)

    def aug_rows(b, ib, s_first):
        r = lax.broadcasted_iota(jnp.int32, (128, TB), 0)
        out = jnp.where((r >= 3 - s_first) & (r < 6 - s_first), 1.0, 0.0)
        for m in range(3):
            out = jnp.where(r == s_first + m, ext_row(b, m, ib), out)
        return out.astype(BF16)

    def charge_row(b, ib):
        return (ext_row(b, 3, ib) + ext_row(b, 4, ib)) + ext_row(b, 5, ib)

    def prep_u(n, _):
        u, ib = n // NB, n % NB
        xt = xe[u, pl.ds(pl.multiple_of(ib * TB, TB), TB), :].T
        xi[n, 0:128, :] = xt
        xi[n, 128:256, :] = aug_rows(u, ib, 3)
        qu[n] = jnp.broadcast_to(charge_row(u, ib), (8, TB))
        return 0

    def prep_v(n, _):
        v, ib = n // NB, n % NB
        b = jnp.where(v == 0, 0, v + GT - 1)
        xb = xe[b, pl.ds(pl.multiple_of(ib * TB, TB), TB), :]
        xv[n, :, 0:128] = xb
        xv[n, :, 128:256] = aug_rows(b, ib, 0).T
        xtv[n] = xb.T
        qv[n] = jnp.broadcast_to(charge_row(b, ib), (128, TB)).T
        sv[n] = jnp.zeros((TB, 128), F32)
        fv[n] = jnp.zeros((128, TB), F32)
        return 0

    lax.fori_loop(0, GT * NB, prep_u, 0)
    lax.fori_loop(0, (HALF_SHELL + 1) * NB, prep_v, 0)

    def run(*accs):
        G = lambda q, k, p: accs[(q * 2 + k) * NP + p]
        F = lambda q, k: accs[4 * NP + q * 2 + k]
        FJ = lambda q, s: accs[4 * NP + 4 + q * 2 + s]

        def issue_g(u, bj, k):
            for q in range(2):
                pltpu.matmul_push_rhs(xi[NB * u + 2 * k + q], staging_register=1, mxu_index=q)
            for p in range(NP):
                lhs = xv[bj, p * PR:(p + 1) * PR, :]
                for q in range(2):
                    pltpu.matmul_acc_lhs(G(q, k, p), lhs, load_staged_rhs=1 if p == 0 else None)

        def elem(u, bj, k, masked):
            cs = [None, None]
            for p in range(NP):
                qvr = qv[bj, p * PR:(p + 1) * PR, :]
                rs = None
                for q in range(2):
                    ib = NB * u + 2 * k + q
                    quv = qu[ib, 0:1, :]
                    g = pltpu.matmul_pop(G(q, k, p))
                    e = jnp.exp2(jnp.minimum(g * scale, 0.0))
                    w0 = (qvr * quv[:, :128]) * e[:, :128]
                    w1 = (qvr * quv[:, 128:]) * e[:, 128:]
                    w = jnp.concatenate([w0, w1], axis=1)
                    if masked:
                        jj = bj * TB + p * PR + lax.broadcasted_iota(jnp.int32, (PR, TB), 0)
                        ii = ib * TB + lax.broadcasted_iota(jnp.int32, (PR, TB), 1)
                        w = jnp.where(jj < ii, w, 0.0)
                        w0, w1 = w[:, :128], w[:, 128:]
                    wsc[q * 2 + k][p * PR:(p + 1) * PR, :] = w.astype(BF16)
                    c = jnp.sum(w.reshape(PR // 8, 8, TB), axis=0)
                    cs[q] = c if cs[q] is None else cs[q] + c
                    rs = w0 + w1 if rs is None else rs + (w0 + w1)
                sv[bj, p * PR:(p + 1) * PR, :] += rs
            for q in range(2):
                su[NB * u + 2 * k + q] += cs[q]

        def force(u, bj, k, s):
            for q in range(2):
                pltpu.matmul_push_rhs(wsc[q * 2 + k][...], staging_register=1, mxu_index=q)
            lhs = xtv[bj]
            for q in range(2):
                pltpu.matmul_acc_lhs(F(q, k), lhs, load_staged_rhs=1)
            for q in range(2):
                pltpu.matmul_push_rhs(wsc[q * 2 + k][...], staging_register=0, mxu_index=q, transpose=True)
            for q in range(2):
                pltpu.matmul_acc_lhs(FJ(q, s), xi[NB * u + 2 * k + q, 0:128, :], load_staged_rhs=0)

        def flush(bj, s):
            fv[bj] += pltpu.matmul_pop(FJ(0, s)) + pltpu.matmul_pop(FJ(1, s))

        def sweep(u, start, count, masked):
            last = start + count - 1
            for k in range(2):
                issue_g(u, start, k)
            for q in range(2):
                wsc[q * 2 + 1][...] = jnp.zeros((TB, TB), BF16)

            def steps(base, unroll):
                for n in range(unroll):
                    bj, s = base + n, n % 2
                    nxt = jnp.minimum(bj + 1, last)
                    prv = jnp.maximum(bj - 1, start)
                    for k in range(2):
                        elem(u, bj, k, masked)
                        force(u, bj if k else prv, 1 - k, s if k else 1 - s)
                        issue_g(u, nxt, k)
                    flush(prv, 1 - s)

            n8 = 0
            if not masked:
                n8 = count // 8

                def body8(h, _):
                    steps(start + 8 * h, 8)
                    return 0
                lax.fori_loop(0, n8, body8, 0)

            def body4(h, _):
                steps(start + 8 * n8 + 4 * h, 4)
                return 0
            lax.fori_loop(0, count // 4 - 2 * n8, body4, 0)
            force(u, last, 1, 1)
            flush(last, 1)
            for k in range(2):
                for q in range(2):
                    for p in range(NP):
                        pltpu.matmul_pop(G(q, k, p))

        def finish(u):
            for k in range(2):
                for q in range(2):
                    n = NB * u + 2 * k + q
                    tot = jnp.sum(su[n], axis=0, keepdims=True)
                    fu[n] = tot * xi[n, 0:128, :].astype(F32) - pltpu.matmul_pop(F(q, k))

        for n in range(GT * NB):
            su[n] = jnp.zeros((8, TB), F32)
        sweep(0, 0, NB, True)
        def host(u, _):
            start = jnp.where((u == 0) | (u > 4), 1, jnp.where(u == 4, flags[1], 0))
            stop = jnp.where(u == 0, HALF_SHELL + flags[0], jnp.where(u > 4, HALF_SHELL, jnp.where(u == 4, HALF_SHELL + flags[1], HALF_SHELL + 1)))
            sweep(u, NB * start, NB * (stop - start), False)
            finish(u)
            return 0
        lax.fori_loop(0, GT, host, 0)

    specs = [pltpu.ACC(q)((PR, TB), F32) for q in range(2) for k in range(2) for p in range(NP)]
    specs += [pltpu.ACC(q)((128, TB), F32) for q in range(2) for k in range(2)]
    specs += [pltpu.ACC(q)((128, TB), F32) for q in range(2) for s in range(2)]
    pl.run_scoped(run, *specs)

    def post_v(n, _):
        tot = jnp.sum(sv[n].T, axis=0, keepdims=True)
        fv[n] = tot * xtv[n].astype(F32) - fv[n]
        return 0
    lax.fori_loop(0, (HALF_SHELL + 1) * NB, post_v, 0)
    total = su[0]
    for n in range(1, GT * NB):
        total = total + su[n]
    en[...] = total


def solution(mesh):
    def per_device(x_own, q_own):
        rows, feat = x_own.shape
        inv_len2 = 1.0 / feat
        grid_a, grid_t = grid_of(lax.axis_index('seg'), lax.axis_index('col'))
        sq = jnp.sum(jnp.square(x_own.astype(F32)), axis=1)
        half = -jnp.minimum(0.5 * sq, 1.7e38)
        ext = [p.reshape(8, 128) for v in (half, q_own) for p in split3(v)]
        block = jnp.concatenate([x_own] + ext, axis=0)
        axes = ('col', 'seg')
        moved = [block]
        moved += [lax.ppermute(block, axes, shift_pairs(0, d)) for d in range(1, GT)]
        moved += [lax.ppermute(block, axes, shift_pairs(d, 0)) for d in range(1, HALF_SHELL + 1)]
        xe = jnp.stack(moved)
        flags = jnp.stack([(grid_a < HALF_SHELL), (grid_t >= GT // 2)]).astype(jnp.int32)
        vm = pl.BlockSpec(memory_space=pltpu.VMEM)
        nu, nv = GT * NB, (HALF_SHELL + 1) * NB
        fu, fv, en = pl.pallas_call(
            functools.partial(pair_kernel, inv_len2 * math.log2(math.e)),
            out_shape=[jax.ShapeDtypeStruct((nu, 128, TB), F32), jax.ShapeDtypeStruct((nv, 128, TB), F32),
                       jax.ShapeDtypeStruct((8, TB), F32)],
            in_specs=[pl.BlockSpec(memory_space=pltpu.SMEM), vm],
            out_specs=[vm, vm, vm],
            scratch_shapes=[pltpu.VMEM((nu, TB, TB), BF16), pltpu.VMEM((nv, TB, TB), BF16),
                            pltpu.VMEM((nv, 128, TB), BF16), pltpu.VMEM((nu, 8, TB), F32),
                            pltpu.VMEM((nv, TB, 128), F32), pltpu.VMEM((nu, 8, TB), F32),
                            pltpu.VMEM((nv, TB, 128), F32)] + [pltpu.VMEM((TB, TB), BF16)] * 4,
            compiler_params=pltpu.CompilerParams(vmem_limit_bytes=56 * 2**20),
            name='pair_tiles',
        )(flags, xe)
        fu = fu.reshape(GT, NB, 128, TB)
        fv = fv.reshape(HALF_SHELL + 1, NB, 128, TB)
        parts = [fu[0], fv[0]]
        parts += [lax.ppermute(fu[d], axes, shift_pairs(0, -d)) for d in range(1, GT)]
        parts += [lax.ppermute(fv[d], axes, shift_pairs(-d, 0)) for d in range(1, HALF_SHELL + 1)]
        force = functools.reduce(jnp.add, parts)
        force = jnp.swapaxes(force, 1, 2).reshape(rows, feat) * inv_len2
        energy = lax.psum(jnp.sum(en), axes)
        return force, energy.reshape(1)

    row_spec = P(ROW_AXES, None)

    def step(x, q):
        with jax.sharding.use_abstract_mesh(mesh.abstract_mesh):
            return jax.shard_map(per_device, mesh=mesh, in_specs=(row_spec, P(ROW_AXES)),
                                 out_specs=(row_spec, P('sys')), check_vma=False)(x, q)
    return step
```

```python
import functools
import math

import jax
import jax.numpy as jnp
from jax import lax
from jax.experimental import pallas as pl
from jax.experimental.pallas import tpu as pltpu
from jax.sharding import PartitionSpec as P

F32 = jnp.float32
BF16 = jnp.bfloat16
ROW_AXES = ('sys', 'seg', 'col')
GA, GT = 16, 8
OWN = 1024
TB = 256
NB = OWN // TB
EXT = 48
PR = 64
NP = TB // PR
HALF = GA // 2
HOST_STEP = (0, 1, 7, 4, 3, 5, 6, 2)
EITHER = -1
MESH = pl.DeviceIdType.MESH

UNITS = [(u, v) for u in range(GT) for v in range(1, HALF)]
UNITS += [(HOST_STEP.index(d), v) for d in (1, 2, 3) for v in (0, HALF)]
UNITS += [(HOST_STEP.index(4), EITHER), (0, HALF)]
UNITS.sort(key=lambda pair: pair[0])
ONCE = (0, HALF)


def grid_of(seg, col):
    z, y, x = seg // 16, (seg // 4) % 4, seg % 4
    ya = y // 2
    yb = (ya + y % 2) % 2
    return (z * 2 + ya) * 2 + col, x * 2 + yb


def device_at(a, t):
    ya, yb = (a // 2) % 2, t % 2
    return {'seg': (a // 4) * 16 + (2 * ya + (ya + yb) % 2) * 4 + t // 2, 'col': a % 2}


def split3(v):
    hi = lax.reduce_precision(v, 8, 7)
    mid = lax.reduce_precision(v - hi, 8, 7)
    lo = lax.reduce_precision(v - hi - mid, 8, 7)
    return [p.astype(BF16) for p in (hi, mid, lo)]


def pick(table, n):
    out = jnp.int32(table[0])
    for k in range(1, len(table)):
        if table[k] != table[k - 1]:
            out = jnp.where(n >= k, table[k], out)
    return out


class Ring:
    def __init__(self):
        self.a, self.t = grid_of(lax.axis_index('seg'), lax.axis_index('col'))

    def peer(self, da, dt):
        return device_at((self.a + da + GA) % GA, (self.t + dt + GT) % GT)

    def enter(self):
        barrier = pltpu.get_barrier_semaphore()
        for d in range(1, GT):
            pl.semaphore_signal(barrier, inc=1, device_id=self.peer(0, d), device_id_type=MESH)
        for d in range(1, GA):
            pl.semaphore_signal(barrier, inc=1, device_id=self.peer(d, 0), device_id_type=MESH)
        pl.semaphore_wait(barrier, GT + GA - 2)


def gather_kernel(blk, xe, own, snd, rcv):
    ring = Ring()
    keep = pltpu.make_async_copy(blk, xe.at[0], own)
    keep.start()
    ring.enter()
    copies = []
    for n in range(1, HALF + 1):
        for slot in ([GT - 1 + n, n] if n < GT else [GT - 1 + n]):
            to = ring.peer(0, -HOST_STEP[slot]) if slot < GT else ring.peer(-(slot - GT + 1), 0)
            copies.append(pltpu.make_async_remote_copy(src_ref=blk, dst_ref=xe.at[slot], send_sem=snd.at[slot],
                                                       recv_sem=rcv.at[slot], device_id=to, device_id_type=MESH))
            copies[-1].start()
    keep.wait()
    for copy in copies:
        copy.wait_recv()
    for copy in copies:
        copy.wait_send()


def reduce_kernel(inv_len2, fu, fv, en, force_out, en_out, rb, er, ec, mine, own, fsnd, frcv, esnd, ercv):
    ring = Ring()
    keep = [pltpu.make_async_copy(f.at[pl.ds(0, NB)], mine.at[n], own.at[n]) for n, f in enumerate((fu, fv))]
    for copy in keep:
        copy.start()
    ring.enter()
    copies = []
    for n in range(1, HALF + 1):
        for slot in ([GT - 1 + n, n] if n < GT else [GT - 1 + n]):
            src = fu.at[pl.ds(NB * slot, NB)] if slot < GT else fv.at[pl.ds(NB * (slot - GT + 1), NB)]
            to = ring.peer(0, HOST_STEP[slot]) if slot < GT else ring.peer(slot - GT + 1, 0)
            copies.append(pltpu.make_async_remote_copy(src_ref=src, dst_ref=rb.at[slot - 1], send_sem=fsnd.at[slot],
                                                       recv_sem=frcv.at[slot], device_id=to, device_id_type=MESH))
            copies[-1].start()

    def spread(ref, me, along_t):
        out = []
        for n in range(1, GT if along_t else GA):
            k = n if along_t else GT + n
            out.append(pltpu.make_async_remote_copy(src_ref=ref.at[me], dst_ref=ref.at[me], send_sem=esnd.at[k],
                                                    recv_sem=ercv.at[k], device_id=ring.peer(0, n) if along_t else ring.peer(n, 0),
                                                    device_id_type=MESH))
        for copy in out:
            copy.start()
        return out

    def fold(r, count):
        total = r[0]
        for n in range(1, count):
            total = total + r[n]
        return total

    er[ring.t] = en[...]
    for copy in keep:
        copy.wait()
    along = spread(er, ring.t, True)
    for copy in along:
        copy.wait_recv()
    ec[ring.a] = fold(er, GT)
    copies[0].wait_recv()
    across = spread(ec, ring.a, False)
    for copy in copies[1:]:
        copy.wait_recv()
    for copy in across:
        copy.wait_recv()
    en_out[...] = fold(ec, GA)

    def all_sum(ib, _):
        out = mine[0, ib] + mine[1, ib]
        for slot in range(GT + HALF - 1):
            out = out + rb[slot, ib]
        force_out[pl.ds(pl.multiple_of(ib * TB, TB), TB), :] = (out * inv_len2).T
        return 0
    lax.fori_loop(0, NB, all_sum, 0)
    for copy in copies + along + across:
        copy.wait_send()


def pair_kernel(scale, place, xe, fu, fv, en, xi, xv, xtv, qu, qv, su, sv, *wsc):
    my_a, my_t = place[0], place[1]
    def ext_row(b, m, ib):
        row = xe[b, OWN + 8 * m:OWN + 8 * (m + 1), :].astype(F32)
        sel = lax.broadcasted_iota(jnp.int32, (8, 128), 0)
        lo = jnp.sum(jnp.where(sel == 2 * ib, row, 0.0), axis=0, keepdims=True)
        hi = jnp.sum(jnp.where(sel == 2 * ib + 1, row, 0.0), axis=0, keepdims=True)
        return jnp.concatenate([lo, hi], axis=1)

    def aug_rows(b, ib, s_first):
        r = lax.broadcasted_iota(jnp.int32, (128, TB), 0)
        out = jnp.where((r >= 3 - s_first) & (r < 6 - s_first), 1.0, 0.0)
        for m in range(3):
            out = jnp.where(r == s_first + m, ext_row(b, m, ib), out)
        return out.astype(BF16)

    def charge_row(b, ib):
        return (ext_row(b, 3, ib) + ext_row(b, 4, ib)) + ext_row(b, 5, ib)

    def prep_u(u):
        def one(ib, _):
            n = u * NB + ib
            xi[n, 0:128, :] = xe[u, pl.ds(pl.multiple_of(ib * TB, TB), TB), :].T
            xi[n, 128:256, :] = aug_rows(u, ib, 3)
            qu[n] = jnp.broadcast_to(charge_row(u, ib), (8, TB))
            su[n] = jnp.zeros((8, TB), F32)
            fu[n] = jnp.zeros((128, TB), F32)
            return 0
        lax.fori_loop(0, NB, one, 0)

    def prep_v(v):
        b = GT - 1 + v if v else 0

        def one(ib, _):
            n = v * NB + ib
            xb = xe[b, pl.ds(pl.multiple_of(ib * TB, TB), TB), :]
            xv[n, :, 0:128] = xb
            xv[n, :, 128:256] = aug_rows(b, ib, 0).T
            xtv[n] = xb.T
            qv[n] = jnp.broadcast_to(charge_row(b, ib), (128, TB)).T
            sv[n] = jnp.zeros((TB, 128), F32)
            fv[n] = jnp.zeros((128, TB), F32)
            return 0
        lax.fori_loop(0, NB, one, 0)

    for n in range(GT):
        prep_u(n)
    for n in range(HALF + 1):
        prep_v(n)


    def finish_u(u):
        def one(ib, _):
            n = u * NB + ib
            fu[n] = jnp.sum(su[n], axis=0, keepdims=True) * xi[n, 0:128, :].astype(F32) - fu[n]
            return 0
        lax.fori_loop(0, NB, one, 0)

    def finish_v(v):
        def one(ib, _):
            n = v * NB + ib
            fv[n] = jnp.sum(sv[n].T, axis=0, keepdims=True) * xtv[n].astype(F32) - fv[n]
            return 0
        lax.fori_loop(0, NB, one, 0)

    def run(*accs):
        G = lambda q, k, p: accs[(q * 2 + k) * NP + p]
        F = lambda q, k: accs[4 * NP + q * 2 + k]
        FJ = lambda q, s: accs[4 * NP + 4 + q * 2 + s]

        def issue_g(u, bj, k):
            for q in range(2):
                pltpu.matmul_push_rhs(xi[NB * u + 2 * k + q], staging_register=1, mxu_index=q)
            for p in range(NP):
                lhs = xv[bj, p * PR:(p + 1) * PR, :]
                for q in range(2):
                    pltpu.matmul_acc_lhs(G(q, k, p), lhs, load_staged_rhs=1 if p == 0 else None)

        def elem(u, bj, k, weight, masked):
            cs = [None, None]
            for p in range(NP):
                qvr = qv[bj, p * PR:(p + 1) * PR, :]
                rs = None
                for q in range(2):
                    ib = NB * u + 2 * k + q
                    quv = qu[ib, 0:1, :] * weight
                    g = pltpu.matmul_pop(G(q, k, p))
                    e = jnp.exp2(jnp.minimum(g * scale, 0.0))
                    w0 = (qvr * quv[:, :128]) * e[:, :128]
                    w1 = (qvr * quv[:, 128:]) * e[:, 128:]
                    w = jnp.concatenate([w0, w1], axis=1)
                    if masked:
                        jj = bj * TB + p * PR + lax.broadcasted_iota(jnp.int32, (PR, TB), 0)
                        ii = ib * TB + lax.broadcasted_iota(jnp.int32, (PR, TB), 1)
                        w = jnp.where(jj < ii, w, 0.0)
                        w0, w1 = w[:, :128], w[:, 128:]
                    wsc[q * 2 + k][p * PR:(p + 1) * PR, :] = w.astype(BF16)
                    c = jnp.sum(w.reshape(PR // 8, 8, TB), axis=0)
                    cs[q] = c if cs[q] is None else cs[q] + c
                    rs = w0 + w1 if rs is None else rs + (w0 + w1)
                sv[bj, p * PR:(p + 1) * PR, :] += rs
            for q in range(2):
                su[NB * u + 2 * k + q] += cs[q]

        def force(u, bj, k, s):
            for q in range(2):
                pltpu.matmul_push_rhs(wsc[q * 2 + k][...], staging_register=1, mxu_index=q)
            lhs = xtv[bj]
            for q in range(2):
                pltpu.matmul_acc_lhs(F(q, k), lhs, load_staged_rhs=1)
            for q in range(2):
                pltpu.matmul_push_rhs(wsc[q * 2 + k][...], staging_register=0, mxu_index=q, transpose=True)
            for q in range(2):
                pltpu.matmul_acc_lhs(FJ(q, s), xi[NB * u + 2 * k + q, 0:128, :], load_staged_rhs=0)

        def flush(bj, s):
            fv[bj] += pltpu.matmul_pop(FJ(0, s)) + pltpu.matmul_pop(FJ(1, s))

        def host_pop(u, k):
            for q in range(2):
                fu[NB * u + 2 * k + q] += pltpu.matmul_pop(F(q, k))

        def unit(prev, cur, nxt, masked):
            weight = 1.0 if masked else jnp.where((cur[0] == ONCE[0]) & (cur[1] == ONCE[1]) & (my_a >= HALF), 0.0, 1.0)
            for n in range(NB):
                bj, s = NB * cur[1] + n, n % 2
                for k in range(2):
                    elem(cur[0], bj, k, weight, masked)
                    if k == 0 and n == 0:
                        force(prev[0], NB * prev[1] + NB - 1, 1, 1)
                        host_pop(prev[0], 0)
                    else:
                        force(cur[0], bj - 1 + k, 1 - k, s if k else 1 - s)
                    if n < NB - 1:
                        issue_g(cur[0], bj + 1, k)
                    elif nxt is not None:
                        issue_g(nxt[0], NB * nxt[1], k)
                if n == 0:
                    host_pop(prev[0], 1)
                    flush(NB * prev[1] + NB - 1, 1)
                else:
                    flush(bj - 1, 1 - s)

        def start(pair):
            for k in range(2):
                issue_g(pair[0], NB * pair[1], k)

        own = (jnp.int32(0), jnp.int32(0))
        for q in range(2):
            wsc[q * 2 + 1][...] = jnp.zeros((TB, TB), BF16)
        either = jnp.where(my_t >= GT // 2, HALF, 0)

        def unit_at(n):
            v = pick([pair[1] for pair in UNITS], n)
            return pick([pair[0] for pair in UNITS], n), jnp.where(v == EITHER, either, v)

        first = unit_at(jnp.int32(0))
        start(own)
        unit(own, own, first, True)

        def two(h, carry):
            prev, cur = carry[:2], carry[2:]
            mid = unit_at(2 * h + 1)
            nxt = unit_at(jnp.minimum(2 * h + 2, len(UNITS) - 1))
            unit(prev, cur, mid, False)
            unit(cur, mid, nxt, False)
            return *mid, *nxt

        last = lax.fori_loop(0, len(UNITS) // 2, two, (*own, *first))[:2]
        force(last[0], NB * last[1] + NB - 1, 1, 1)
        for k in range(2):
            for q in range(2):
                for p in range(NP):
                    pltpu.matmul_pop(G(q, k, p))
        flush(NB * last[1] + NB - 1, 1)
        for k in range(2):
            host_pop(last[0], k)

    specs = [pltpu.ACC(q)((PR, TB), F32) for q in range(2) for k in range(2) for p in range(NP)]
    specs += [pltpu.ACC(q)((128, TB), F32) for q in range(2) for k in range(2)]
    specs += [pltpu.ACC(q)((128, TB), F32) for q in range(2) for s in range(2)]
    pl.run_scoped(run, *specs)
    total = jnp.zeros((8, TB), F32)
    for n in range(GT * NB):
        total = total + su[n]
    en[...] = total[:, :128] + total[:, 128:]
    for n in range(GT):
        finish_u(n)
    for n in range(HALF + 1):
        finish_v(n)


def solution(mesh):
    def per_device(x_own, q_own):
        rows, feat = x_own.shape
        inv_len2 = 1.0 / feat
        sq = jnp.sum(jnp.square(x_own.astype(F32)), axis=1)
        half = -jnp.minimum(0.5 * sq, 1.7e38)
        ext = [p.reshape(8, 128) for v in (half, q_own) for p in split3(v)]
        block = jnp.concatenate([x_own] + ext, axis=0)
        vm, hbm = pl.BlockSpec(memory_space=pltpu.VMEM), pl.BlockSpec(memory_space=pl.ANY)
        nu, nv, nr = GT * NB, (HALF + 1) * NB, GT + HALF
        dma = pltpu.SemaphoreType.DMA
        shape = jax.ShapeDtypeStruct
        xe = pl.pallas_call(
            gather_kernel, out_shape=shape((nr, OWN + EXT, 128), BF16), in_specs=[vm], out_specs=hbm,
            scratch_shapes=[dma(()), dma((nr,)), dma((nr,))],
            compiler_params=pltpu.CompilerParams(collective_id=0, has_side_effects=True), name='gather_blocks',
        )(block)
        place = jnp.stack(grid_of(lax.axis_index('seg'), lax.axis_index('col'))).astype(jnp.int32)
        fu, fv, en = pl.pallas_call(
            functools.partial(pair_kernel, inv_len2 * math.log2(math.e)),
            out_shape=[shape((nu, 128, TB), F32), shape((nv, 128, TB), F32), shape((8, 128), F32)],
            in_specs=[pl.BlockSpec(memory_space=pltpu.SMEM), vm],
            out_specs=[vm, vm, vm],
            scratch_shapes=[pltpu.VMEM((nu, TB, TB), BF16), pltpu.VMEM((nv, TB, TB), BF16),
                            pltpu.VMEM((nv, 128, TB), BF16), pltpu.VMEM((nu, 8, TB), F32),
                            pltpu.VMEM((nv, TB, 128), F32), pltpu.VMEM((nu, 8, TB), F32),
                            pltpu.VMEM((nv, TB, 128), F32)] + [pltpu.VMEM((TB, TB), BF16)] * 4,
            compiler_params=pltpu.CompilerParams(vmem_limit_bytes=48 * 2**20),
            name='pair_tiles',
        )(place, xe)
        force, en = pl.pallas_call(
            functools.partial(reduce_kernel, inv_len2),
            out_shape=[shape((rows, feat), F32), shape((8, 128), F32)],
            in_specs=[hbm, hbm, vm], out_specs=[vm, vm],
            scratch_shapes=[pltpu.VMEM((nr - 1, NB, 128, TB), F32), pltpu.VMEM((GT, 8, 128), F32),
                            pltpu.VMEM((GA, 8, 128), F32), pltpu.VMEM((2, NB, 128, TB), F32), dma((2,)),
                            dma((nr,)), dma((nr,)), dma((GT + GA,)), dma((GT + GA,))],
            compiler_params=pltpu.CompilerParams(collective_id=1, has_side_effects=True), name='reduce_forces',
        )(fu, fv, en)
        return force, jnp.sum(en).reshape(1)

    row_spec = P(ROW_AXES, None)

    def step(x, q):
        with jax.sharding.use_abstract_mesh(mesh.abstract_mesh):
            return jax.shard_map(per_device, mesh=mesh, in_specs=(row_spec, P(ROW_AXES)),
                                 out_specs=(row_spec, P('sys')), check_vma=False)(x, q)
    return step
```

```python
import functools
import math

import jax
import jax.numpy as jnp
from jax import lax
from jax.experimental import pallas as pl
from jax.experimental.pallas import tpu as pltpu
from jax.sharding import PartitionSpec as P

F32 = jnp.float32
BF16 = jnp.bfloat16
ROW_AXES = ('sys', 'seg', 'col')
GA, GT = 16, 8
OWN = 1024
TB = 256
NB = OWN // TB
EXT = 48
PR = 64
NP = TB // PR
HALF = GA // 2
HOST_STEP = (0, 1, 7, 4, 3, 5, 6, 2)
EITHER = -1
MESH = pl.DeviceIdType.MESH

UNITS = [(u, v) for u in range(GT) for v in range(1, HALF)]
UNITS += [(HOST_STEP.index(d), v) for d in (1, 2, 3) for v in (0, HALF)]
UNITS += [(HOST_STEP.index(4), EITHER), (0, HALF)]
UNITS.sort(key=lambda pair: pair[0])
ONCE = (0, HALF)


def grid_of(seg, col):
    z, y, x = seg // 16, (seg // 4) % 4, seg % 4
    ya = y // 2
    yb = (ya + y % 2) % 2
    return (col * 2 + ya) * 4 + z, x * 2 + yb


def device_at(a, t):
    ya, yb = (a // 4) % 2, t % 2
    return {'seg': (a % 4) * 16 + (2 * ya + (ya + yb) % 2) * 4 + t // 2, 'col': a // 8}


def split3(v):
    hi = lax.reduce_precision(v, 8, 7)
    mid = lax.reduce_precision(v - hi, 8, 7)
    lo = lax.reduce_precision(v - hi - mid, 8, 7)
    return [p.astype(BF16) for p in (hi, mid, lo)]


def pick(table, n):
    out = jnp.int32(table[0])
    for k in range(1, len(table)):
        if table[k] != table[k - 1]:
            out = jnp.where(n >= k, table[k], out)
    return out


class Ring:
    def __init__(self):
        self.a, self.t = grid_of(lax.axis_index('seg'), lax.axis_index('col'))

    def peer(self, da, dt):
        return device_at((self.a + da + GA) % GA, (self.t + dt + GT) % GT)

    def enter(self):
        barrier = pltpu.get_barrier_semaphore()
        for d in range(1, GT):
            pl.semaphore_signal(barrier, inc=1, device_id=self.peer(0, d), device_id_type=MESH)
        for d in range(1, GA):
            pl.semaphore_signal(barrier, inc=1, device_id=self.peer(d, 0), device_id_type=MESH)
        pl.semaphore_wait(barrier, GT + GA - 2)


def gather_kernel(blk, xe, own, snd, rcv):
    ring = Ring()
    keep = pltpu.make_async_copy(blk, xe.at[0], own)
    keep.start()
    ring.enter()
    copies = []
    for n in range(1, HALF + 1):
        for slot in ([GT - 1 + n, n] if n < GT else [GT - 1 + n]):
            to = ring.peer(0, -HOST_STEP[slot]) if slot < GT else ring.peer(-(slot - GT + 1), 0)
            copies.append(pltpu.make_async_remote_copy(src_ref=blk, dst_ref=xe.at[slot], send_sem=snd.at[slot],
                                                       recv_sem=rcv.at[slot], device_id=to, device_id_type=MESH))
            copies[-1].start()
    keep.wait()
    for copy in copies:
        copy.wait_recv()
    for copy in copies:
        copy.wait_send()


def reduce_kernel(inv_len2, fu, fv, en, force_out, en_out, rb, er, ec, mine, own, fsnd, frcv, esnd, ercv):
    ring = Ring()
    keep = [pltpu.make_async_copy(f.at[pl.ds(0, NB)], mine.at[n], own.at[n]) for n, f in enumerate((fu, fv))]
    for copy in keep:
        copy.start()
    ring.enter()
    copies = []
    for n in range(1, HALF + 1):
        for slot in ([GT - 1 + n, n] if n < GT else [GT - 1 + n]):
            src = fu.at[pl.ds(NB * slot, NB)] if slot < GT else fv.at[pl.ds(NB * (slot - GT + 1), NB)]
            to = ring.peer(0, HOST_STEP[slot]) if slot < GT else ring.peer(slot - GT + 1, 0)
            copies.append(pltpu.make_async_remote_copy(src_ref=src, dst_ref=rb.at[slot - 1], send_sem=fsnd.at[slot],
                                                       recv_sem=frcv.at[slot], device_id=to, device_id_type=MESH))
            copies[-1].start()

    def spread(ref, me, along_t):
        out = []
        for n in range(1, GT if along_t else GA):
            k = n if along_t else GT + n
            out.append(pltpu.make_async_remote_copy(src_ref=ref.at[me], dst_ref=ref.at[me], send_sem=esnd.at[k],
                                                    recv_sem=ercv.at[k], device_id=ring.peer(0, n) if along_t else ring.peer(n, 0),
                                                    device_id_type=MESH))
        for copy in out:
            copy.start()
        return out

    def fold(r, count):
        total = r[0]
        for n in range(1, count):
            total = total + r[n]
        return total

    er[ring.t] = en[...]
    for copy in keep:
        copy.wait()
    along = spread(er, ring.t, True)
    for copy in along:
        copy.wait_recv()
    ec[ring.a] = fold(er, GT)
    copies[0].wait_recv()
    across = spread(ec, ring.a, False)
    for copy in copies[1:]:
        copy.wait_recv()
    for copy in across:
        copy.wait_recv()
    en_out[...] = fold(ec, GA)

    def all_sum(ib, _):
        out = mine[0, ib] + mine[1, ib]
        for slot in range(GT + HALF - 1):
            out = out + rb[slot, ib]
        force_out[pl.ds(pl.multiple_of(ib * TB, TB), TB), :] = (out * inv_len2).T
        return 0
    lax.fori_loop(0, NB, all_sum, 0)
    for copy in copies + along + across:
        copy.wait_send()


def pair_kernel(scale, place, xe, fu, fv, en, xi, xv, xtv, qu, qv, su, sv, *wsc):
    my_a, my_t = place[0], place[1]
    def ext_row(b, m, ib):
        row = xe[b, OWN + 8 * m:OWN + 8 * (m + 1), :].astype(F32)
        sel = lax.broadcasted_iota(jnp.int32, (8, 128), 0)
        lo = jnp.sum(jnp.where(sel == 2 * ib, row, 0.0), axis=0, keepdims=True)
        hi = jnp.sum(jnp.where(sel == 2 * ib + 1, row, 0.0), axis=0, keepdims=True)
        return jnp.concatenate([lo, hi], axis=1)

    def aug_rows(b, ib, s_first):
        r = lax.broadcasted_iota(jnp.int32, (128, TB), 0)
        out = jnp.where((r >= 3 - s_first) & (r < 6 - s_first), 1.0, 0.0)
        for m in range(3):
            out = jnp.where(r == s_first + m, ext_row(b, m, ib), out)
        return out.astype(BF16)

    def charge_row(b, ib):
        return (ext_row(b, 3, ib) + ext_row(b, 4, ib)) + ext_row(b, 5, ib)

    def prep_u(u):
        def one(ib, _):
            n = u * NB + ib
            xi[n, 0:128, :] = xe[u, pl.ds(pl.multiple_of(ib * TB, TB), TB), :].T
            xi[n, 128:256, :] = aug_rows(u, ib, 3)
            qu[n] = jnp.broadcast_to(charge_row(u, ib), (8, TB))
            su[n] = jnp.zeros((8, TB), F32)
            fu[n] = jnp.zeros((128, TB), F32)
            return 0
        lax.fori_loop(0, NB, one, 0)

    def prep_v(v):
        b = GT - 1 + v if v else 0

        def one(ib, _):
            n = v * NB + ib
            xb = xe[b, pl.ds(pl.multiple_of(ib * TB, TB), TB), :]
            xv[n, :, 0:128] = xb
            xv[n, :, 128:256] = aug_rows(b, ib, 0).T
            xtv[n] = xb.T
            qv[n] = jnp.broadcast_to(charge_row(b, ib), (128, TB)).T
            sv[n] = jnp.zeros((TB, 128), F32)
            fv[n] = jnp.zeros((128, TB), F32)
            return 0
        lax.fori_loop(0, NB, one, 0)

    for n in range(GT):
        prep_u(n)
    for n in range(HALF + 1):
        prep_v(n)


    def finish_u(u):
        def one(ib, _):
            n = u * NB + ib
            fu[n] = jnp.sum(su[n], axis=0, keepdims=True) * xi[n, 0:128, :].astype(F32) - fu[n]
            return 0
        lax.fori_loop(0, NB, one, 0)

    def finish_v(v):
        def one(ib, _):
            n = v * NB + ib
            fv[n] = jnp.sum(sv[n].T, axis=0, keepdims=True) * xtv[n].astype(F32) - fv[n]
            return 0
        lax.fori_loop(0, NB, one, 0)

    def run(*accs):
        G = lambda q, k, p: accs[(q * 2 + k) * NP + p]
        F = lambda q, k: accs[4 * NP + q * 2 + k]
        FJ = lambda q, s: accs[4 * NP + 4 + q * 2 + s]

        def issue_g(u, bj, k):
            for q in range(2):
                pltpu.matmul_push_rhs(xi[NB * u + 2 * k + q], staging_register=1, mxu_index=q)
            for p in range(NP):
                lhs = xv[bj, p * PR:(p + 1) * PR, :]
                for q in range(2):
                    pltpu.matmul_acc_lhs(G(q, k, p), lhs, load_staged_rhs=1 if p == 0 else None)

        def elem(u, bj, k, weight, masked):
            cs = [None, None]
            for p in range(NP):
                qvr = qv[bj, p * PR:(p + 1) * PR, :]
                rs = None
                for q in range(2):
                    ib = NB * u + 2 * k + q
                    quv = qu[ib, 0:1, :] * weight
                    g = pltpu.matmul_pop(G(q, k, p))
                    e = jnp.exp2(jnp.minimum(g * scale, 0.0))
                    w0 = (qvr * quv[:, :128]) * e[:, :128]
                    w1 = (qvr * quv[:, 128:]) * e[:, 128:]
                    w = jnp.concatenate([w0, w1], axis=1)
                    if masked:
                        jj = bj * TB + p * PR + lax.broadcasted_iota(jnp.int32, (PR, TB), 0)
                        ii = ib * TB + lax.broadcasted_iota(jnp.int32, (PR, TB), 1)
                        w = jnp.where(jj < ii, w, 0.0)
                        w0, w1 = w[:, :128], w[:, 128:]
                    wsc[q * 2 + k][p * PR:(p + 1) * PR, :] = w.astype(BF16)
                    c = jnp.sum(w.reshape(PR // 8, 8, TB), axis=0)
                    cs[q] = c if cs[q] is None else cs[q] + c
                    rs = w0 + w1 if rs is None else rs + (w0 + w1)
                sv[bj, p * PR:(p + 1) * PR, :] += rs
            for q in range(2):
                su[NB * u + 2 * k + q] += cs[q]

        def force(u, bj, k, s):
            for q in range(2):
                pltpu.matmul_push_rhs(wsc[q * 2 + k][...], staging_register=1, mxu_index=q)
            lhs = xtv[bj]
            for q in range(2):
                pltpu.matmul_acc_lhs(F(q, k), lhs, load_staged_rhs=1)
            for q in range(2):
                pltpu.matmul_push_rhs(wsc[q * 2 + k][...], staging_register=0, mxu_index=q, transpose=True)
            for q in range(2):
                pltpu.matmul_acc_lhs(FJ(q, s), xi[NB * u + 2 * k + q, 0:128, :], load_staged_rhs=0)

        def flush(bj, s):
            fv[bj] += pltpu.matmul_pop(FJ(0, s)) + pltpu.matmul_pop(FJ(1, s))

        def host_pop(u, k):
            for q in range(2):
                fu[NB * u + 2 * k + q] += pltpu.matmul_pop(F(q, k))

        def unit(prev, cur, nxt, masked):
            weight = 1.0 if masked else jnp.where((cur[0] == ONCE[0]) & (cur[1] == ONCE[1]) & (my_a >= HALF), 0.0, 1.0)
            for n in range(NB):
                bj, s = NB * cur[1] + n, n % 2
                for k in range(2):
                    elem(cur[0], bj, k, weight, masked)
                    if k == 0 and n == 0:
                        force(prev[0], NB * prev[1] + NB - 1, 1, 1)
                        host_pop(prev[0], 0)
                    else:
                        force(cur[0], bj - 1 + k, 1 - k, s if k else 1 - s)
                    if n < NB - 1:
                        issue_g(cur[0], bj + 1, k)
                    elif nxt is not None:
                        issue_g(nxt[0], NB * nxt[1], k)
                if n == 0:
                    host_pop(prev[0], 1)
                    flush(NB * prev[1] + NB - 1, 1)
                else:
                    flush(bj - 1, 1 - s)

        def start(pair):
            for k in range(2):
                issue_g(pair[0], NB * pair[1], k)

        own = (jnp.int32(0), jnp.int32(0))
        for q in range(2):
            wsc[q * 2 + 1][...] = jnp.zeros((TB, TB), BF16)
        either = jnp.where(my_t >= GT // 2, HALF, 0)

        def unit_at(n):
            v = pick([pair[1] for pair in UNITS], n)
            return pick([pair[0] for pair in UNITS], n), jnp.where(v == EITHER, either, v)

        first = unit_at(jnp.int32(0))
        start(own)
        unit(own, own, first, True)

        def two(h, carry):
            prev, cur = carry[:2], carry[2:]
            mid = unit_at(2 * h + 1)
            nxt = unit_at(jnp.minimum(2 * h + 2, len(UNITS) - 1))
            unit(prev, cur, mid, False)
            unit(cur, mid, nxt, False)
            return *mid, *nxt

        last = lax.fori_loop(0, len(UNITS) // 2, two, (*own, *first))[:2]
        force(last[0], NB * last[1] + NB - 1, 1, 1)
        for k in range(2):
            for q in range(2):
                for p in range(NP):
                    pltpu.matmul_pop(G(q, k, p))
        flush(NB * last[1] + NB - 1, 1)
        for k in range(2):
            host_pop(last[0], k)

    specs = [pltpu.ACC(q)((PR, TB), F32) for q in range(2) for k in range(2) for p in range(NP)]
    specs += [pltpu.ACC(q)((128, TB), F32) for q in range(2) for k in range(2)]
    specs += [pltpu.ACC(q)((128, TB), F32) for q in range(2) for s in range(2)]
    pl.run_scoped(run, *specs)
    total = jnp.zeros((8, TB), F32)
    for n in range(GT * NB):
        total = total + su[n]
    en[...] = total[:, :128] + total[:, 128:]
    for n in range(GT):
        finish_u(n)
    for n in range(HALF + 1):
        finish_v(n)


def solution(mesh):
    def per_device(x_own, q_own):
        rows, feat = x_own.shape
        inv_len2 = 1.0 / feat
        sq = jnp.sum(jnp.square(x_own.astype(F32)), axis=1)
        half = -jnp.minimum(0.5 * sq, 1.7e38)
        ext = [p.reshape(8, 128) for v in (half, q_own) for p in split3(v)]
        block = jnp.concatenate([x_own] + ext, axis=0)
        vm, hbm = pl.BlockSpec(memory_space=pltpu.VMEM), pl.BlockSpec(memory_space=pl.ANY)
        nu, nv, nr = GT * NB, (HALF + 1) * NB, GT + HALF
        dma = pltpu.SemaphoreType.DMA
        shape = jax.ShapeDtypeStruct
        xe = pl.pallas_call(
            gather_kernel, out_shape=shape((nr, OWN + EXT, 128), BF16), in_specs=[vm], out_specs=hbm,
            scratch_shapes=[dma(()), dma((nr,)), dma((nr,))],
            compiler_params=pltpu.CompilerParams(collective_id=0, has_side_effects=True), name='gather_blocks',
        )(block)
        place = jnp.stack(grid_of(lax.axis_index('seg'), lax.axis_index('col'))).astype(jnp.int32)
        fu, fv, en = pl.pallas_call(
            functools.partial(pair_kernel, inv_len2 * math.log2(math.e)),
            out_shape=[shape((nu, 128, TB), F32), shape((nv, 128, TB), F32), shape((8, 128), F32)],
            in_specs=[pl.BlockSpec(memory_space=pltpu.SMEM), vm],
            out_specs=[vm, vm, vm],
            scratch_shapes=[pltpu.VMEM((nu, TB, TB), BF16), pltpu.VMEM((nv, TB, TB), BF16),
                            pltpu.VMEM((nv, 128, TB), BF16), pltpu.VMEM((nu, 8, TB), F32),
                            pltpu.VMEM((nv, TB, 128), F32), pltpu.VMEM((nu, 8, TB), F32),
                            pltpu.VMEM((nv, TB, 128), F32)] + [pltpu.VMEM((TB, TB), BF16)] * 4,
            compiler_params=pltpu.CompilerParams(vmem_limit_bytes=48 * 2**20),
            name='pair_tiles',
        )(place, xe)
        force, en = pl.pallas_call(
            functools.partial(reduce_kernel, inv_len2),
            out_shape=[shape((rows, feat), F32), shape((8, 128), F32)],
            in_specs=[hbm, hbm, vm], out_specs=[vm, vm],
            scratch_shapes=[pltpu.VMEM((nr - 1, NB, 128, TB), F32), pltpu.VMEM((GT, 8, 128), F32),
                            pltpu.VMEM((GA, 8, 128), F32), pltpu.VMEM((2, NB, 128, TB), F32), dma((2,)),
                            dma((nr,)), dma((nr,)), dma((GT + GA,)), dma((GT + GA,))],
            compiler_params=pltpu.CompilerParams(collective_id=1, has_side_effects=True), name='reduce_forces',
        )(fu, fv, en)
        return force, jnp.sum(en).reshape(1)

    row_spec = P(ROW_AXES, None)

    def step(x, q):
        with jax.sharding.use_abstract_mesh(mesh.abstract_mesh):
            return jax.shard_map(per_device, mesh=mesh, in_specs=(row_spec, P(ROW_AXES)),
                                 out_specs=(row_spec, P('sys')), check_vma=False)(x, q)
    return step
```

```python
import functools
import math

import jax
import jax.numpy as jnp
from jax import lax
from jax.experimental import pallas as pl
from jax.experimental.pallas import tpu as pltpu
from jax.sharding import PartitionSpec as P

F32 = jnp.float32
BF16 = jnp.bfloat16
ROW_AXES = ('sys', 'seg', 'col')
GA, GT = 16, 8
OWN = 1024
TB = 256
NB = OWN // TB
LANES, SUB, NEXT = 128, 8, 2
EXT = 48
PR = 64
NP = TB // PR
HALF = GA // 2
EITHER = -1
MESH = pl.DeviceIdType.MESH

UNITS = [(u, v) for u in range(GT) for v in range(1, HALF)]
UNITS += [(u, v) for u in (1, 2, 3) for v in (0, HALF)]
UNITS += [(4, EITHER), (0, HALF)]
UNITS.sort(key=lambda pair: pair[0])
ONCE = (0, HALF)


def grid_of(seg, col):
    z, y, x = seg // 16, (seg // 4) % 4, seg % 4
    ya = y // 2
    yb = (ya + y % 2) % 2
    return (col * 2 + ya) * 4 + z, x * 2 + yb


def device_at(a, t):
    ya, yb = (a // 4) % 2, t % 2
    return {'seg': (a % 4) * 16 + (2 * ya + (ya + yb) % 2) * 4 + t // 2, 'col': a // 8}


def pick(table, n):
    out = jnp.int32(table[0])
    for k in range(1, len(table)):
        if table[k] != table[k - 1]:
            out = jnp.where(n >= k, table[k], out)
    return out


class Ring:
    def __init__(self):
        self.a, self.t = grid_of(lax.axis_index('seg'), lax.axis_index('col'))
        self.flip = 1 - 2 * (self.t % 2)

    def peer(self, da, dt):
        return device_at((self.a + da + GA) % GA, (self.t + dt + GT) % GT)

    def enter(self):
        barrier = pltpu.get_barrier_semaphore()
        for d in range(1, GT):
            pl.semaphore_signal(barrier, inc=1, device_id=self.peer(0, d), device_id_type=MESH)
        for d in range(1, GA):
            pl.semaphore_signal(barrier, inc=1, device_id=self.peer(d, 0), device_id_type=MESH)
        pl.semaphore_wait(barrier, GT + GA - 2)


def split3(v):
    parts = []
    for _ in range(3):
        parts.append(v.astype(BF16))
        v = v - parts[-1].astype(F32)
    return parts


def gather_kernel(x, q, xe, blk, half, own, snd, rcv):
    ring = Ring()
    flip = ring.flip
    blk[0:OWN, :] = x[...]
    for r in range(OWN // LANES):
        rows = x[r * LANES:(r + 1) * LANES, :].astype(F32)
        half[r:r + 1, :] = jnp.sum((rows * rows).T, axis=0, keepdims=True)
    for n, part in enumerate(split3(-jnp.minimum(0.5 * half[...], 1.7e38)) + split3(q[...])):
        blk[OWN + SUB * n:OWN + SUB * (n + 1), :] = part

    def slot_u(dx):
        return (2 * dx + flip + GT) % GT

    def slot_v(d):
        return GT - 1 + d

    copies = []

    def copy(src, slot, a=0, t=0):
        m = len(copies)
        copies.append(pltpu.make_async_remote_copy(src_ref=src, dst_ref=xe.at[slot], send_sem=snd.at[m], recv_sem=rcv.at[m],
                                                   device_id=ring.peer(a, t), device_id_type=MESH))
        return copies[-1]

    right, left = -NEXT % GT, NEXT
    own_right, own_left = copy(blk, right, t=NEXT), copy(blk, left, t=-NEXT)
    own_over = copy(blk, (GT - flip) % GT, t=flip)
    pass_right = copy(xe.at[right], 2 * NEXT, t=NEXT)
    over = xe.at[slot_u(0)]
    over_right, over_left = copy(over, slot_u(-1), t=NEXT), copy(over, slot_u(1), t=-NEXT)
    over_pass = copy(xe.at[slot_u(1)], slot_u(2), t=-NEXT)
    direct = {d: copy(blk, slot_v(d), a=-d) for d in range(1, HALF + 1) if d % 4 != 2}
    pass_down = copy(xe.at[slot_v(1)], slot_v(2), a=-1)
    pass_up = copy(xe.at[slot_v(7)], slot_v(6), a=1)
    ring.enter()
    keep = pltpu.make_async_copy(blk, xe.at[0], own)
    keep.start()
    for c in (own_over, own_right, own_left, direct[1], direct[7], direct[4], direct[3], direct[5], direct[8]):
        c.start()
    through = ((own_over, (over_right, over_left)), (own_right, (pass_right,)), (direct[1], (pass_down,)),
               (direct[7], (pass_up,)), (over_left, (over_pass,)))
    for got, then in through:
        got.wait_recv()
        for c in then:
            c.start()
    for c in copies:
        if all(c is not got for got, _ in through):
            c.wait_recv()
    for c in copies:
        c.wait_send()
    keep.wait()


def reduce_kernel(inv_len2, fu, fv, en, force_out, en_out, rb, er, ec, fsnd, frcv, esnd, ercv):
    ring = Ring()
    flip = ring.flip

    def same(dx):
        return pl.multiple_of(NB * ((2 * dx + GT) % GT), NB)

    def other(dx):
        return pl.multiple_of(NB * ((2 * dx + flip + GT) % GT), NB)

    copies = []

    def copy(src, first, a=0, t=0):
        m = len(copies)
        src = src if first is None else src.at[pl.ds(first, NB)]
        copies.append(pltpu.make_async_remote_copy(src_ref=src, dst_ref=rb.at[m], send_sem=fsnd.at[m], recv_sem=frcv.at[m],
                                                   device_id=ring.peer(a, t), device_id_type=MESH))
        return m

    far_o, far_s = copy(fu, other(2), t=-NEXT), copy(fu, same(2), t=NEXT)
    near_o, near_s = copy(fu, other(1), t=NEXT), copy(fu, same(-1), t=-NEXT)
    sum_o, sum_s = copy(rb.at[far_o], None, t=-NEXT), copy(rb.at[far_s], None, t=NEXT)
    over = copy(rb.at[near_o], None, t=flip)
    up, down = copy(fv, NB * 2, a=1), copy(fv, NB * 6, a=-1)
    direct = [copy(fv, NB * d, a=d) for d in (4, 3, 5, 8)]
    sum_up, sum_down = copy(rb.at[up], None, a=1), copy(rb.at[down], None, a=7)

    def spread(ref, me, along_t):
        out = []
        for n in range(1, GT if along_t else GA):
            k = n if along_t else GT + n
            out.append(pltpu.make_async_remote_copy(src_ref=ref.at[me], dst_ref=ref.at[me], send_sem=esnd.at[k], recv_sem=ercv.at[k],
                                                    device_id=ring.peer(*((0, n) if along_t else (n, 0))), device_id_type=MESH))
        for c in out:
            c.start()
        return out

    def fold(r, count):
        total = r[0]
        for n in range(1, count):
            total = total + r[n]
        return total

    def add(m, ref, first):
        copies[m].wait_recv()

        def one(ib, _):
            rb[m, ib] = rb[m, ib] + ref[first + ib]
            return 0
        lax.fori_loop(0, NB, one, 0)

    er[ring.t] = en[...]
    ring.enter()
    for m in (far_o, up, down, far_s, near_o, direct[0], near_s, *direct[1:]):
        copies[m].start()
    along = spread(er, ring.t, True)
    for c in along:
        c.wait_recv()
    ec[ring.a] = fold(er, GT)
    add(far_o, fu, other(-1))
    add(up, fv, NB)
    copies[sum_o].start()
    add(down, fv, NB * 7)
    copies[sum_up].start()
    add(far_s, fu, same(1))
    copies[sum_down].start()
    across = spread(ec, ring.a, False)
    copies[sum_s].start()
    copies[sum_o].wait_recv()
    copies[near_o].wait_recv()

    def beside(ib, _):
        rb[near_o, ib] = rb[near_o, ib] + rb[sum_o, ib] + fu[other(0) + ib]
        return 0
    lax.fori_loop(0, NB, beside, 0)
    for c in across:
        c.wait_recv()
    en_out[0] = jnp.sum(fold(ec, GA))
    copies[over].start()
    late = (near_s, sum_s, *direct, sum_up, sum_down, over)
    for m in late:
        copies[m].wait_recv()

    def all_sum(ib, _):
        out = fu[ib] + fv[ib]
        for m in late:
            out = out + rb[m, ib]
        force_out[pl.ds(pl.multiple_of(ib * TB, TB), TB), :] = (out * inv_len2).T
        return 0
    lax.fori_loop(0, NB, all_sum, 0)
    for c in [*copies, *along, *across]:
        c.wait_send()


def pair_kernel(scale, place, xe, fu, fv, en, xi, xv, xtv, qu, qv, su, sv, *wsc):
    my_a, my_t = place[0], place[1]
    def ext_row(b, m, ib):
        row = xe[b, OWN + 8 * m:OWN + 8 * (m + 1), :].astype(F32)
        sel = lax.broadcasted_iota(jnp.int32, (8, 128), 0)
        lo = jnp.sum(jnp.where(sel == 2 * ib, row, 0.0), axis=0, keepdims=True)
        hi = jnp.sum(jnp.where(sel == 2 * ib + 1, row, 0.0), axis=0, keepdims=True)
        return jnp.concatenate([lo, hi], axis=1)

    def aug_rows(b, ib, s_first):
        r = lax.broadcasted_iota(jnp.int32, (128, TB), 0)
        out = jnp.where((r >= 3 - s_first) & (r < 6 - s_first), 1.0, 0.0)
        for m in range(3):
            out = jnp.where(r == s_first + m, ext_row(b, m, ib), out)
        return out.astype(BF16)

    def charge_row(b, ib):
        return (ext_row(b, 3, ib) + ext_row(b, 4, ib)) + ext_row(b, 5, ib)

    def prep_u(u):
        def one(ib, _):
            n = u * NB + ib
            xi[n, 0:128, :] = xe[u, pl.ds(pl.multiple_of(ib * TB, TB), TB), :].T
            xi[n, 128:256, :] = aug_rows(u, ib, 3)
            qu[n] = jnp.broadcast_to(charge_row(u, ib), (8, TB))
            su[n] = jnp.zeros((8, TB), F32)
            fu[n] = jnp.zeros((128, TB), F32)
            return 0
        lax.fori_loop(0, NB, one, 0)

    def prep_v(v):
        b = GT - 1 + v if v else 0

        def one(ib, _):
            n = v * NB + ib
            xb = xe[b, pl.ds(pl.multiple_of(ib * TB, TB), TB), :]
            xv[n, :, 0:128] = xb
            xv[n, :, 128:256] = aug_rows(b, ib, 0).T
            xtv[n] = xb.T
            qv[n] = jnp.broadcast_to(charge_row(b, ib), (128, TB)).T
            sv[n] = jnp.zeros((TB, 128), F32)
            fv[n] = jnp.zeros((128, TB), F32)
            return 0
        lax.fori_loop(0, NB, one, 0)

    for n in range(GT):
        prep_u(n)
    for n in range(HALF + 1):
        prep_v(n)


    def finish_u(u):
        def one(ib, _):
            n = u * NB + ib
            fu[n] = jnp.sum(su[n], axis=0, keepdims=True) * xi[n, 0:128, :].astype(F32) - fu[n]
            return 0
        lax.fori_loop(0, NB, one, 0)

    def finish_v(v):
        def one(ib, _):
            n = v * NB + ib
            fv[n] = jnp.sum(sv[n].T, axis=0, keepdims=True) * xtv[n].astype(F32) - fv[n]
            return 0
        lax.fori_loop(0, NB, one, 0)

    def run(*accs):
        G = lambda q, k, p: accs[(q * 2 + k) * NP + p]
        F = lambda q, k: accs[4 * NP + q * 2 + k]
        FJ = lambda q, s: accs[4 * NP + 4 + q * 2 + s]

        def issue_g(u, bj, k):
            for q in range(2):
                pltpu.matmul_push_rhs(xi[NB * u + 2 * k + q], staging_register=1, mxu_index=q)
            for p in range(NP):
                lhs = xv[bj, p * PR:(p + 1) * PR, :]
                for q in range(2):
                    pltpu.matmul_acc_lhs(G(q, k, p), lhs, load_staged_rhs=1 if p == 0 else None)

        def elem(u, bj, k, weight, masked):
            cs = [None, None]
            for p in range(NP):
                qvr = qv[bj, p * PR:(p + 1) * PR, :]
                rs = None
                for q in range(2):
                    ib = NB * u + 2 * k + q
                    quv = qu[ib, 0:1, :] * weight
                    g = pltpu.matmul_pop(G(q, k, p))
                    e = jnp.exp2(jnp.minimum(g * scale, 0.0))
                    w0 = (qvr * quv[:, :128]) * e[:, :128]
                    w1 = (qvr * quv[:, 128:]) * e[:, 128:]
                    w = jnp.concatenate([w0, w1], axis=1)
                    if masked:
                        jj = bj * TB + p * PR + lax.broadcasted_iota(jnp.int32, (PR, TB), 0)
                        ii = ib * TB + lax.broadcasted_iota(jnp.int32, (PR, TB), 1)
                        w = jnp.where(jj < ii, w, 0.0)
                        w0, w1 = w[:, :128], w[:, 128:]
                    wsc[q * 2 + k][p * PR:(p + 1) * PR, :] = w.astype(BF16)
                    c = jnp.sum(w.reshape(PR // 8, 8, TB), axis=0)
                    cs[q] = c if cs[q] is None else cs[q] + c
                    rs = w0 + w1 if rs is None else rs + (w0 + w1)
                sv[bj, p * PR:(p + 1) * PR, :] += rs
            for q in range(2):
                su[NB * u + 2 * k + q] += cs[q]

        def force(u, bj, k, s):
            for q in range(2):
                pltpu.matmul_push_rhs(wsc[q * 2 + k][...], staging_register=1, mxu_index=q)
            lhs = xtv[bj]
            for q in range(2):
                pltpu.matmul_acc_lhs(F(q, k), lhs, load_staged_rhs=1)
            for q in range(2):
                pltpu.matmul_push_rhs(wsc[q * 2 + k][...], staging_register=0, mxu_index=q, transpose=True)
            for q in range(2):
                pltpu.matmul_acc_lhs(FJ(q, s), xi[NB * u + 2 * k + q, 0:128, :], load_staged_rhs=0)

        def flush(bj, s):
            fv[bj] += pltpu.matmul_pop(FJ(0, s)) + pltpu.matmul_pop(FJ(1, s))

        def host_pop(u, k):
            for q in range(2):
                fu[NB * u + 2 * k + q] += pltpu.matmul_pop(F(q, k))

        def unit(prev, cur, nxt, masked):
            weight = 1.0 if masked else jnp.where((cur[0] == ONCE[0]) & (cur[1] == ONCE[1]) & (my_a >= HALF), 0.0, 1.0)
            for n in range(NB):
                bj, s = NB * cur[1] + n, n % 2
                for k in range(2):
                    elem(cur[0], bj, k, weight, masked)
                    if k == 0 and n == 0:
                        force(prev[0], NB * prev[1] + NB - 1, 1, 1)
                        host_pop(prev[0], 0)
                    else:
                        force(cur[0], bj - 1 + k, 1 - k, s if k else 1 - s)
                    if n < NB - 1:
                        issue_g(cur[0], bj + 1, k)
                    elif nxt is not None:
                        issue_g(nxt[0], NB * nxt[1], k)
                if n == 0:
                    host_pop(prev[0], 1)
                    flush(NB * prev[1] + NB - 1, 1)
                else:
                    flush(bj - 1, 1 - s)

        def start(pair):
            for k in range(2):
                issue_g(pair[0], NB * pair[1], k)

        own = (jnp.int32(0), jnp.int32(0))
        for q in range(2):
            wsc[q * 2 + 1][...] = jnp.zeros((TB, TB), BF16)
        either = jnp.where(my_t >= GT // 2, HALF, 0)

        def unit_at(n):
            v = pick([pair[1] for pair in UNITS], n)
            return pick([pair[0] for pair in UNITS], n), jnp.where(v == EITHER, either, v)

        first = unit_at(jnp.int32(0))
        start(own)
        unit(own, own, first, True)

        def two(h, carry):
            prev, cur = carry[:2], carry[2:]
            mid = unit_at(2 * h + 1)
            nxt = unit_at(jnp.minimum(2 * h + 2, len(UNITS) - 1))
            unit(prev, cur, mid, False)
            unit(cur, mid, nxt, False)
            return *mid, *nxt

        last = lax.fori_loop(0, len(UNITS) // 2, two, (*own, *first))[:2]
        force(last[0], NB * last[1] + NB - 1, 1, 1)
        for k in range(2):
            for q in range(2):
                for p in range(NP):
                    pltpu.matmul_pop(G(q, k, p))
        flush(NB * last[1] + NB - 1, 1)
        for k in range(2):
            host_pop(last[0], k)

    specs = [pltpu.ACC(q)((PR, TB), F32) for q in range(2) for k in range(2) for p in range(NP)]
    specs += [pltpu.ACC(q)((128, TB), F32) for q in range(2) for k in range(2)]
    specs += [pltpu.ACC(q)((128, TB), F32) for q in range(2) for s in range(2)]
    pl.run_scoped(run, *specs)
    total = jnp.zeros((8, TB), F32)
    for n in range(GT * NB):
        total = total + su[n]
    en[...] = total[:, :128] + total[:, 128:]
    for n in range(GT):
        finish_u(n)
    for n in range(HALF + 1):
        finish_v(n)


def solution(mesh):
    def per_device(x_own, q_own):
        rows, feat = x_own.shape
        inv_len2 = 1.0 / feat
        vm, hbm = pl.BlockSpec(memory_space=pltpu.VMEM), pl.BlockSpec(memory_space=pl.ANY)
        nu, nv, nr = GT * NB, (HALF + 1) * NB, GT + HALF
        dma = pltpu.SemaphoreType.DMA
        shape = jax.ShapeDtypeStruct
        xe = pl.pallas_call(
            gather_kernel, out_shape=shape((nr, OWN + EXT, 128), BF16), in_specs=[vm, vm], out_specs=hbm,
            scratch_shapes=[pltpu.VMEM((OWN + EXT, LANES), BF16), pltpu.VMEM((SUB, LANES), F32), dma(()), dma((nr,)), dma((nr,))],
            compiler_params=pltpu.CompilerParams(collective_id=0, has_side_effects=True), name='gather_blocks',
        )(x_own, q_own.reshape(SUB, LANES))
        place = jnp.stack(grid_of(lax.axis_index('seg'), lax.axis_index('col'))).astype(jnp.int32)
        fu, fv, en = pl.pallas_call(
            functools.partial(pair_kernel, inv_len2 * math.log2(math.e)),
            out_shape=[shape((nu, 128, TB), F32), shape((nv, 128, TB), F32), shape((8, 128), F32)],
            in_specs=[pl.BlockSpec(memory_space=pltpu.SMEM), vm],
            out_specs=[vm, vm, vm],
            scratch_shapes=[pltpu.VMEM((nu, TB, TB), BF16), pltpu.VMEM((nv, TB, TB), BF16),
                            pltpu.VMEM((nv, 128, TB), BF16), pltpu.VMEM((nu, 8, TB), F32),
                            pltpu.VMEM((nv, TB, 128), F32), pltpu.VMEM((nu, 8, TB), F32),
                            pltpu.VMEM((nv, TB, 128), F32)] + [pltpu.VMEM((TB, TB), BF16)] * 4,
            compiler_params=pltpu.CompilerParams(vmem_limit_bytes=48 * 2**20),
            name='pair_tiles',
        )(place, xe)
        force, en = pl.pallas_call(
            functools.partial(reduce_kernel, inv_len2),
            out_shape=[shape((rows, feat), F32), shape((1,), F32)],
            in_specs=[vm, vm, vm], out_specs=[vm, pl.BlockSpec(memory_space=pltpu.SMEM)],
            scratch_shapes=[pltpu.VMEM((nr - 1, NB, 128, TB), F32), pltpu.VMEM((GT, 8, 128), F32),
                            pltpu.VMEM((GA, 8, 128), F32), dma((nr,)), dma((nr,)), dma((GT + GA,)), dma((GT + GA,))],
            compiler_params=pltpu.CompilerParams(vmem_limit_bytes=32 * 2**20, collective_id=1, has_side_effects=True), name='reduce_forces',
        )(fu, fv, en)
        return force, en

    row_spec = P(ROW_AXES, None)

    def step(x, q):
        with jax.sharding.use_abstract_mesh(mesh.abstract_mesh):
            return jax.shard_map(per_device, mesh=mesh, in_specs=(row_spec, P(ROW_AXES)),
                                 out_specs=(row_spec, P('sys')), check_vma=False)(x, q)
    return step
```

```python
import functools
import math

import jax
import jax.numpy as jnp
from jax import lax
from jax.experimental import pallas as pl
from jax.experimental.pallas import tpu as pltpu
from jax.sharding import PartitionSpec as P

F32 = jnp.float32
BF16 = jnp.bfloat16
ROW_AXES = ('sys', 'seg', 'col')
GA, GT = 16, 8
OWN = 1024
TB = 256
NB = OWN // TB
LANES, SUB, NEXT = 128, 8, 2
EXT = 48
PR = 64
NP = TB // PR
HALF = GA // 2
EITHER = -1
MESH = pl.DeviceIdType.MESH

UNITS = [(u, v) for u in range(GT) for v in range(1, HALF)]
UNITS += [(u, v) for u in (1, 2, 3) for v in (0, HALF)]
UNITS += [(4, EITHER), (0, HALF)]
UNITS.sort(key=lambda pair: pair[0])
ONCE = (0, HALF)


def grid_of(seg, col):
    z, y, x = seg // 16, (seg // 4) % 4, seg % 4
    ya = y // 2
    yb = (ya + y % 2) % 2
    return (col * 2 + ya) * 4 + z, x * 2 + yb


def device_at(a, t):
    ya, yb = (a // 4) % 2, t % 2
    return {'seg': (a % 4) * 16 + (2 * ya + (ya + yb) % 2) * 4 + t // 2, 'col': a // 8}


def pick(table, n):
    out = jnp.int32(table[0])
    for k in range(1, len(table)):
        if table[k] != table[k - 1]:
            out = jnp.where(n >= k, table[k], out)
    return out


class Ring:
    def __init__(self):
        self.a, self.t = grid_of(lax.axis_index('seg'), lax.axis_index('col'))
        self.flip = 1 - 2 * (self.t % 2)

    def peer(self, da, dt):
        return device_at((self.a + da + GA) % GA, (self.t + dt + GT) % GT)

    def enter(self):
        barrier = pltpu.get_barrier_semaphore()
        for d in range(1, GT):
            pl.semaphore_signal(barrier, inc=1, device_id=self.peer(0, d), device_id_type=MESH)
        for d in range(1, GA):
            pl.semaphore_signal(barrier, inc=1, device_id=self.peer(d, 0), device_id_type=MESH)
        pl.semaphore_wait(barrier, GT + GA - 2)


def split3(v):
    parts = []
    for _ in range(3):
        parts.append(v.astype(BF16))
        v = v - parts[-1].astype(F32)
    return parts


def gather_kernel(x, q, xe, blk, half, snd, rcv):
    ring = Ring()
    flip = ring.flip
    blk[0:OWN, :] = x[...]
    for r in range(OWN // LANES):
        rows = x[r * LANES:(r + 1) * LANES, :].astype(F32)
        half[r:r + 1, :] = jnp.sum((rows * rows).T, axis=0, keepdims=True)
    for n, part in enumerate(split3(-jnp.minimum(0.5 * half[...], 1.7e38)) + split3(q[...])):
        blk[OWN + SUB * n:OWN + SUB * (n + 1), :] = part

    def slot_u(dx):
        return (2 * dx + flip + GT) % GT

    def slot_v(d):
        return GT - 1 + d

    copies = []

    def copy(src, slot, a=0, t=0):
        m = len(copies)
        copies.append(pltpu.make_async_remote_copy(src_ref=src, dst_ref=xe.at[slot], send_sem=snd.at[m], recv_sem=rcv.at[m],
                                                   device_id=ring.peer(a, t), device_id_type=MESH))
        return copies[-1]

    right, left = -NEXT % GT, NEXT
    own_right, own_left = copy(blk, right, t=NEXT), copy(blk, left, t=-NEXT)
    own_over = copy(blk, (GT - flip) % GT, t=flip)
    pass_right = copy(xe.at[right], 2 * NEXT, t=NEXT)
    over = xe.at[slot_u(0)]
    over_right, over_left = copy(over, slot_u(-1), t=NEXT), copy(over, slot_u(1), t=-NEXT)
    over_pass = copy(xe.at[slot_u(1)], slot_u(2), t=-NEXT)
    direct = {d: copy(blk, slot_v(d), a=-d) for d in range(1, HALF + 1) if d % 4 != 2}
    pass_down = copy(xe.at[slot_v(1)], slot_v(2), a=-1)
    pass_up = copy(xe.at[slot_v(7)], slot_v(6), a=1)
    ring.enter()
    for c in (own_over, own_right, own_left, direct[1], direct[7], direct[4], direct[3], direct[5], direct[8]):
        c.start()
    through = ((own_over, (over_right, over_left)), (own_right, (pass_right,)), (direct[1], (pass_down,)),
               (direct[7], (pass_up,)), (over_left, (over_pass,)))
    for got, then in through:
        got.wait_recv()
        for c in then:
            c.start()
    for c in copies:
        if all(c is not got for got, _ in through):
            c.wait_recv()
    xe[0] = blk[...]
    for c in copies:
        c.wait_send()


def reduce_kernel(inv_len2, fu, fv, en, force_out, en_out, rb, er, ec, fsnd, frcv, esnd, ercv):
    ring = Ring()
    flip = ring.flip

    def same(dx):
        return pl.multiple_of(NB * ((2 * dx + GT) % GT), NB)

    def other(dx):
        return pl.multiple_of(NB * ((2 * dx + flip + GT) % GT), NB)

    copies = []

    def copy(src, first, a=0, t=0):
        m = len(copies)
        src = src if first is None else src.at[pl.ds(first, NB)]
        copies.append(pltpu.make_async_remote_copy(src_ref=src, dst_ref=rb.at[m], send_sem=fsnd.at[m], recv_sem=frcv.at[m],
                                                   device_id=ring.peer(a, t), device_id_type=MESH))
        return m

    far_o, far_s = copy(fu, other(2), t=-NEXT), copy(fu, same(2), t=NEXT)
    near_o, near_s = copy(fu, other(1), t=NEXT), copy(fu, same(-1), t=-NEXT)
    sum_o, sum_s = copy(rb.at[far_o], None, t=-NEXT), copy(rb.at[far_s], None, t=NEXT)
    over = copy(rb.at[near_o], None, t=flip)
    up, down = copy(fv, NB * 2, a=1), copy(fv, NB * 6, a=-1)
    direct = [copy(fv, NB * d, a=d) for d in (4, 3, 5, 8)]
    sum_up, sum_down = copy(rb.at[up], None, a=1), copy(rb.at[down], None, a=7)

    def spread(ref, me, along_t):
        out = []
        for n in range(1, GT if along_t else GA):
            k = n if along_t else GT + n
            out.append(pltpu.make_async_remote_copy(src_ref=ref.at[me], dst_ref=ref.at[me], send_sem=esnd.at[k], recv_sem=ercv.at[k],
                                                    device_id=ring.peer(*((0, n) if along_t else (n, 0))), device_id_type=MESH))
        for c in out:
            c.start()
        return out

    def fold(r, count):
        total = r[0]
        for n in range(1, count):
            total = total + r[n]
        return total

    def add(m, ref, first):
        copies[m].wait_recv()

        def one(ib, _):
            rb[m, ib] = rb[m, ib] + ref[first + ib]
            return 0
        lax.fori_loop(0, NB, one, 0)

    er[ring.t] = en[...]
    ring.enter()
    for m in (far_o, up, down, far_s, near_o, *direct):
        copies[m].start()
    along = spread(er, ring.t, True)
    add(far_o, fu, other(-1))
    for c in along:
        c.wait_recv()
    ec[ring.a] = fold(er, GT)
    copies[sum_o].start()
    copies[near_s].start()
    add(up, fv, NB)
    add(down, fv, NB * 7)
    copies[sum_up].start()
    add(far_s, fu, same(1))
    copies[sum_down].start()
    across = spread(ec, ring.a, False)
    copies[sum_s].start()
    copies[sum_o].wait_recv()
    copies[near_o].wait_recv()

    def beside(ib, _):
        rb[near_o, ib] = rb[near_o, ib] + rb[sum_o, ib] + fu[other(0) + ib]
        return 0
    lax.fori_loop(0, NB, beside, 0)
    for c in across:
        c.wait_recv()
    en_out[0] = jnp.sum(fold(ec, GA))
    copies[over].start()
    late = (near_s, sum_s, *direct, sum_up, sum_down, over)
    for m in late:
        copies[m].wait_recv()

    def all_sum(ib, _):
        out = fu[ib] + fv[ib]
        for m in late:
            out = out + rb[m, ib]
        force_out[pl.ds(pl.multiple_of(ib * TB, TB), TB), :] = (out * inv_len2).T
        return 0
    lax.fori_loop(0, NB, all_sum, 0)
    for c in [*copies, *along, *across]:
        c.wait_send()


def pair_kernel(scale, place, xe, fu, fv, en, xi, xv, xtv, qu, qv, su, sv, *wsc):
    my_a, my_t = place[0], place[1]
    def ext_row(b, m, ib):
        row = xe[b, OWN + 8 * m:OWN + 8 * (m + 1), :].astype(F32)
        sel = lax.broadcasted_iota(jnp.int32, (8, 128), 0)
        lo = jnp.sum(jnp.where(sel == 2 * ib, row, 0.0), axis=0, keepdims=True)
        hi = jnp.sum(jnp.where(sel == 2 * ib + 1, row, 0.0), axis=0, keepdims=True)
        return jnp.concatenate([lo, hi], axis=1)

    def aug_rows(b, ib, s_first):
        r = lax.broadcasted_iota(jnp.int32, (128, TB), 0)
        out = jnp.where((r >= 3 - s_first) & (r < 6 - s_first), 1.0, 0.0)
        for m in range(3):
            out = jnp.where(r == s_first + m, ext_row(b, m, ib), out)
        return out.astype(BF16)

    def charge_row(b, ib):
        return (ext_row(b, 3, ib) + ext_row(b, 4, ib)) + ext_row(b, 5, ib)

    def prep_u(u):
        def one(ib, _):
            n = u * NB + ib
            xi[n, 0:128, :] = xe[u, pl.ds(pl.multiple_of(ib * TB, TB), TB), :].T
            xi[n, 128:256, :] = aug_rows(u, ib, 3)
            qu[n] = jnp.broadcast_to(charge_row(u, ib), (8, TB))
            su[n] = jnp.zeros((8, TB), F32)
            fu[n] = jnp.zeros((128, TB), F32)
            return 0
        lax.fori_loop(0, NB, one, 0)

    def prep_v(v):
        b = GT - 1 + v if v else 0

        def one(ib, _):
            n = v * NB + ib
            xb = xe[b, pl.ds(pl.multiple_of(ib * TB, TB), TB), :]
            xv[n, :, 0:128] = xb
            xv[n, :, 128:256] = aug_rows(b, ib, 0).T
            xtv[n] = xb.T
            qv[n] = jnp.broadcast_to(charge_row(b, ib), (128, TB)).T
            sv[n] = jnp.zeros((TB, 128), F32)
            fv[n] = jnp.zeros((128, TB), F32)
            return 0
        lax.fori_loop(0, NB, one, 0)

    for n in range(GT):
        prep_u(n)
    for n in range(HALF + 1):
        prep_v(n)


    def finish_u(u):
        def one(ib, _):
            n = u * NB + ib
            fu[n] = jnp.sum(su[n], axis=0, keepdims=True) * xi[n, 0:128, :].astype(F32) - fu[n]
            return 0
        lax.fori_loop(0, NB, one, 0)

    def finish_v(v):
        def one(ib, _):
            n = v * NB + ib
            fv[n] = jnp.sum(sv[n].T, axis=0, keepdims=True) * xtv[n].astype(F32) - fv[n]
            return 0
        lax.fori_loop(0, NB, one, 0)

    def run(*accs):
        G = lambda q, k, p: accs[(q * 2 + k) * NP + p]
        F = lambda q, k: accs[4 * NP + q * 2 + k]
        FJ = lambda q, s: accs[4 * NP + 4 + q * 2 + s]

        def issue_g(u, bj, k):
            for q in range(2):
                pltpu.matmul_push_rhs(xi[NB * u + 2 * k + q], staging_register=1, mxu_index=q)
            for p in range(NP):
                lhs = xv[bj, p * PR:(p + 1) * PR, :]
                for q in range(2):
                    pltpu.matmul_acc_lhs(G(q, k, p), lhs, load_staged_rhs=1 if p == 0 else None)

        def elem(u, bj, k, weight, masked):
            cs = [None, None]
            for p in range(NP):
                qvr = qv[bj, p * PR:(p + 1) * PR, :]
                rs = None
                for q in range(2):
                    ib = NB * u + 2 * k + q
                    quv = qu[ib, 0:1, :] * weight
                    g = pltpu.matmul_pop(G(q, k, p))
                    e = jnp.exp2(jnp.minimum(g * scale, 0.0))
                    w0 = (qvr * quv[:, :128]) * e[:, :128]
                    w1 = (qvr * quv[:, 128:]) * e[:, 128:]
                    w = jnp.concatenate([w0, w1], axis=1)
                    if masked:
                        jj = bj * TB + p * PR + lax.broadcasted_iota(jnp.int32, (PR, TB), 0)
                        ii = ib * TB + lax.broadcasted_iota(jnp.int32, (PR, TB), 1)
                        w = jnp.where(jj < ii, w, 0.0)
                        w0, w1 = w[:, :128], w[:, 128:]
                    wsc[q * 2 + k][p * PR:(p + 1) * PR, :] = w.astype(BF16)
                    c = jnp.sum(w.reshape(PR // 8, 8, TB), axis=0)
                    cs[q] = c if cs[q] is None else cs[q] + c
                    rs = w0 + w1 if rs is None else rs + (w0 + w1)
                sv[bj, p * PR:(p + 1) * PR, :] += rs
            for q in range(2):
                su[NB * u + 2 * k + q] += cs[q]

        def force(u, bj, k, s):
            for q in range(2):
                pltpu.matmul_push_rhs(wsc[q * 2 + k][...], staging_register=1, mxu_index=q)
            lhs = xtv[bj]
            for q in range(2):
                pltpu.matmul_acc_lhs(F(q, k), lhs, load_staged_rhs=1)
            for q in range(2):
                pltpu.matmul_push_rhs(wsc[q * 2 + k][...], staging_register=0, mxu_index=q, transpose=True)
            for q in range(2):
                pltpu.matmul_acc_lhs(FJ(q, s), xi[NB * u + 2 * k + q, 0:128, :], load_staged_rhs=0)

        def flush(bj, s):
            fv[bj] += pltpu.matmul_pop(FJ(0, s)) + pltpu.matmul_pop(FJ(1, s))

        def host_pop(u, k):
            for q in range(2):
                fu[NB * u + 2 * k + q] += pltpu.matmul_pop(F(q, k))

        def unit(prev, cur, nxt, masked):
            weight = 1.0 if masked else jnp.where((cur[0] == ONCE[0]) & (cur[1] == ONCE[1]) & (my_a >= HALF), 0.0, 1.0)
            for n in range(NB):
                bj, s = NB * cur[1] + n, n % 2
                for k in range(2):
                    elem(cur[0], bj, k, weight, masked)
                    if k == 0 and n == 0:
                        force(prev[0], NB * prev[1] + NB - 1, 1, 1)
                        host_pop(prev[0], 0)
                    else:
                        force(cur[0], bj - 1 + k, 1 - k, s if k else 1 - s)
                    if n < NB - 1:
                        issue_g(cur[0], bj + 1, k)
                    elif nxt is not None:
                        issue_g(nxt[0], NB * nxt[1], k)
                if n == 0:
                    host_pop(prev[0], 1)
                    flush(NB * prev[1] + NB - 1, 1)
                else:
                    flush(bj - 1, 1 - s)

        def start(pair):
            for k in range(2):
                issue_g(pair[0], NB * pair[1], k)

        own = (jnp.int32(0), jnp.int32(0))
        for q in range(2):
            wsc[q * 2 + 1][...] = jnp.zeros((TB, TB), BF16)
        either = jnp.where(my_t >= GT // 2, HALF, 0)

        def unit_at(n):
            v = pick([pair[1] for pair in UNITS], n)
            return pick([pair[0] for pair in UNITS], n), jnp.where(v == EITHER, either, v)

        first = unit_at(jnp.int32(0))
        start(own)
        unit(own, own, first, True)

        def two(h, carry):
            prev, cur = carry[:2], carry[2:]
            mid = unit_at(2 * h + 1)
            nxt = unit_at(jnp.minimum(2 * h + 2, len(UNITS) - 1))
            unit(prev, cur, mid, False)
            unit(cur, mid, nxt, False)
            return *mid, *nxt

        last = lax.fori_loop(0, len(UNITS) // 2, two, (*own, *first))[:2]
        force(last[0], NB * last[1] + NB - 1, 1, 1)
        for k in range(2):
            for q in range(2):
                for p in range(NP):
                    pltpu.matmul_pop(G(q, k, p))
        flush(NB * last[1] + NB - 1, 1)
        for k in range(2):
            host_pop(last[0], k)

    specs = [pltpu.ACC(q)((PR, TB), F32) for q in range(2) for k in range(2) for p in range(NP)]
    specs += [pltpu.ACC(q)((128, TB), F32) for q in range(2) for k in range(2)]
    specs += [pltpu.ACC(q)((128, TB), F32) for q in range(2) for s in range(2)]
    pl.run_scoped(run, *specs)
    total = jnp.zeros((8, TB), F32)
    for n in range(GT * NB):
        total = total + su[n]
    en[...] = total[:, :128] + total[:, 128:]
    for n in range(GT):
        finish_u(n)
    for n in range(HALF + 1):
        finish_v(n)


def solution(mesh):
    def per_device(x_own, q_own):
        rows, feat = x_own.shape
        inv_len2 = 1.0 / feat
        vm = pl.BlockSpec(memory_space=pltpu.VMEM)
        nu, nv, nr = GT * NB, (HALF + 1) * NB, GT + HALF
        dma = pltpu.SemaphoreType.DMA
        shape = jax.ShapeDtypeStruct
        xe = pl.pallas_call(
            gather_kernel, out_shape=shape((nr, OWN + EXT, 128), BF16), in_specs=[vm, vm], out_specs=vm,
            scratch_shapes=[pltpu.VMEM((OWN + EXT, LANES), BF16), pltpu.VMEM((SUB, LANES), F32), dma((nr,)), dma((nr,))],
            compiler_params=pltpu.CompilerParams(vmem_limit_bytes=12 * 2**20, collective_id=0, has_side_effects=True), name='gather_blocks',
        )(x_own, q_own.reshape(SUB, LANES))
        place = jnp.stack(grid_of(lax.axis_index('seg'), lax.axis_index('col'))).astype(jnp.int32)
        fu, fv, en = pl.pallas_call(
            functools.partial(pair_kernel, inv_len2 * math.log2(math.e)),
            out_shape=[shape((nu, 128, TB), F32), shape((nv, 128, TB), F32), shape((8, 128), F32)],
            in_specs=[pl.BlockSpec(memory_space=pltpu.SMEM), vm],
            out_specs=[vm, vm, vm],
            scratch_shapes=[pltpu.VMEM((nu, TB, TB), BF16), pltpu.VMEM((nv, TB, TB), BF16),
                            pltpu.VMEM((nv, 128, TB), BF16), pltpu.VMEM((nu, 8, TB), F32),
                            pltpu.VMEM((nv, TB, 128), F32), pltpu.VMEM((nu, 8, TB), F32),
                            pltpu.VMEM((nv, TB, 128), F32)] + [pltpu.VMEM((TB, TB), BF16)] * 4,
            compiler_params=pltpu.CompilerParams(vmem_limit_bytes=38 * 2**20),
            name='pair_tiles',
        )(place, xe)
        force, en = pl.pallas_call(
            functools.partial(reduce_kernel, inv_len2),
            out_shape=[shape((rows, feat), F32), shape((1,), F32)],
            in_specs=[vm, vm, vm], out_specs=[vm, pl.BlockSpec(memory_space=pltpu.SMEM)],
            scratch_shapes=[pltpu.VMEM((nr - 1, NB, 128, TB), F32), pltpu.VMEM((GT, 8, 128), F32),
                            pltpu.VMEM((GA, 8, 128), F32), dma((nr,)), dma((nr,)), dma((GT + GA,)), dma((GT + GA,))],
            compiler_params=pltpu.CompilerParams(vmem_limit_bytes=20 * 2**20, collective_id=1, has_side_effects=True), name='reduce_forces',
        )(fu, fv, en)
        return force, en

    row_spec = P(ROW_AXES, None)

    def step(x, q):
        with jax.sharding.use_abstract_mesh(mesh.abstract_mesh):
            return jax.shard_map(per_device, mesh=mesh, in_specs=(row_spec, P(ROW_AXES)),
                                 out_specs=(row_spec, P('sys')), check_vma=False)(x, q)
    return step
```
